32 devices in a mesh: dp: 8 (over z, x), mp: 4 (over y, core).
Axes of the slice: x: 2, y: 2, z: 4, core: 2. Of those that a mesh axis runs over, the one named last changes fastest.
Arguments:
- acts: bfloat16 [1, 16384, 4096], P(None, 'dp'), may hold values from -64 to 64
- out_grads: bfloat16 [1, 16384, 4096], P(None, 'dp', 'mp'), may hold values from -80 to 80
- clip_bound: float32 [1], replicated, may hold values from 163840 to 491520
- noise: float32 [1, 4096, 4096], P(None, 'dp', 'mp'), may hold values from -6 to 6
Outputs:
- update: float32 [1, 4096, 4096], P(None, 'dp', 'mp')
The draws below stay inside these ranges and needn't reach their ends.
All inputs are finite; a program needn't handle non-finite values.
Results may differ from the reference program's by a relative error of at most 0.0017.
Values may be sent and summed in bfloat16 or wider, within the bound.
A program may use at most 128 MiB of HBM per device.

```python
import math
import jax
import jax.numpy as jnp
from jax import lax

D = 4096
GROUPS = 1
SEQ = 512
BATCH = 32
TOKENS = 16384


def token_signs(key):
    sign_key = jax.random.fold_in(key, 37)
    flips = jax.random.bernoulli(sign_key, 0.5, (GROUPS, BATCH, SEQ, 1))
    return jnp.where(flips, 1.0, -1.0).astype(jnp.float32)


def draw_acts(key, part):
    base_key = jax.random.fold_in(key, 11)
    key_rows, key_cols, key_base = jax.random.split(base_key, 3)
    key_direction = jax.random.fold_in(base_key, 5)
    row_scale = jnp.exp(jax.random.uniform(key_rows, (GROUPS, TOKENS, 1), jnp.float32, math.log(0.3), math.log(3.0)))
    col_scale = jnp.exp(jax.random.uniform(key_cols, (GROUPS, 1, D), jnp.float32, math.log(0.3), math.log(3.0)))
    direction = jnp.clip(jax.random.normal(key_direction, (GROUPS, BATCH, 1, D), jnp.float32), -2.5, 2.5)
    shared = (0.35 * token_signs(key) * direction).reshape(GROUPS, TOKENS, D)
    base_draw = jnp.clip(jax.random.normal(key_base, (GROUPS, TOKENS, D), jnp.float32), -6.0, 6.0)
    return ((base_draw + shared) * row_scale * col_scale).astype(jnp.bfloat16)


def draw_out_grads(key, part):
    base_key = jax.random.fold_in(key, 23)
    key_examples, key_rows, key_cols, key_base = jax.random.split(base_key, 4)
    key_direction = jax.random.fold_in(base_key, 7)
    example_scale = jnp.exp(jax.random.uniform(key_examples, (GROUPS, BATCH, 1, 1), jnp.float32, math.log(0.3), math.log(3.0)))
    row_scale = jnp.exp(jax.random.uniform(key_rows, (GROUPS, BATCH, SEQ, 1), jnp.float32, math.log(0.5), math.log(2.0)))
    col_scale = jnp.exp(jax.random.uniform(key_cols, (GROUPS, 1, 1, D), jnp.float32, math.log(0.5), math.log(2.0)))
    direction = jnp.clip(jax.random.normal(key_direction, (GROUPS, BATCH, 1, D), jnp.float32), -2.5, 2.5)
    shared = 0.25 * token_signs(key) * direction
    base_draw = jnp.clip(jax.random.normal(key_base, (GROUPS, BATCH, SEQ, D), jnp.float32), -6.0, 6.0)
    values = (base_draw + shared) * example_scale * row_scale * col_scale
    return values.reshape(GROUPS, TOKENS, D).astype(jnp.bfloat16)


def block_scale(rng, dims, cuts, smallest, largest):
    factor_of = 1.0
    for position, blocks in cuts:
        heights = jax.random.uniform(jax.random.fold_in(jax.random.fold_in(rng, 6), position), (blocks,), jnp.float32, smallest / len(cuts), largest / len(cuts))
        factor_of = factor_of * jnp.repeat(jnp.exp(heights), dims[position] // blocks).reshape((-1,) + (1,) * (len(dims) - 1 - position))
    return factor_of


def bell_draw(rng, shape, spread, reach, pieces=(), held_as=jnp.bfloat16):
    values = spread * jax.random.normal(rng, shape, jnp.float32)
    if pieces:
        values = values * block_scale(rng, shape, pieces, -0.22, 0.18)
    return jnp.clip(values, -reach, reach).astype(held_as)


def setup_inputs(seed: int = 0) -> dict:
    key_of = jax.random.split(jax.random.key(seed), 5)
    acts = draw_acts(jax.random.fold_in(key_of[4], 71), 0)
    out_grads = draw_out_grads(jax.random.fold_in(key_of[4], 71), 0)
    clip_bound = jnp.clip(jnp.exp(jax.random.uniform(key_of[2], (GROUPS,), jnp.float32, math.log(163840.0), math.log(491520.0))), 163840.0, 491520.0)
    noise = bell_draw(key_of[3], (GROUPS, D, D), 0.5, 6.0, ((1, 8), (2, 4)), jnp.float32)
    return {"acts": acts, "out_grads": out_grads, "clip_bound": clip_bound, "noise": noise}


def reference(acts, out_grads, clip_bound, noise):
    results = []
    for group_index in range(GROUPS):
        act_seq = acts[group_index].reshape(BATCH, SEQ, D)
        grad_seq = out_grads[group_index].reshape(BATCH, SEQ, D)

        def one_example(pair):
            act_one, grad_one = pair
            gram_act = jnp.dot(act_one, act_one.T, preferred_element_type=jnp.float32)
            gram_grad = jnp.dot(grad_one, grad_one.T, preferred_element_type=jnp.float32)
            return jnp.sum(gram_act * gram_grad)
        norm_sq = lax.map(one_example, (act_seq, grad_seq))
        bound = clip_bound[group_index]
        clip = jnp.minimum(1.0, bound / jnp.sqrt(norm_sq + 1e-06))
        factor = clip / bound
        scaled = (grad_seq.astype(jnp.float32) * factor[:, None, None]).astype(jnp.bfloat16)
        scaled = scaled.reshape(TOKENS, D)
        summed = jnp.dot(acts[group_index].T, scaled, preferred_element_type=jnp.float32)
        results.append(summed * (D / math.sqrt(BATCH)) + noise[group_index])
    return jnp.stack(results)
```

```python
import functools
import math

import jax
import jax.numpy as jnp
from jax import lax
from jax.experimental import pallas as pl
from jax.experimental.pallas import tpu as pltpu
from jax.sharding import PartitionSpec as P

SEQ = 512
PIECES = 4
NT = (((1,), (1,)), ((), ()))
MESH = pl.DeviceIdType.MESH
LIFT = 2.0**50


def coded(value):
    lifted = value * LIFT
    return (lifted * jnp.abs(lifted)).astype(jnp.bfloat16)


def decoded(code):
    code = code.astype(jnp.float32)
    return code * lax.rsqrt(jnp.maximum(jnp.abs(code), 1e-37)) * (1.0 / LIFT)


def kernel(
    groups, lanes, share, acts_hbm, grads_hbm, bound_ref, out_hbm,
    acts, grads, grads_t, xs, xr, zs, zr, fr, gram_mine, gram_peer, norm_mine, norm_peer, total, out,
    load_sem, out_sem, gram_send, gram_recv, norm_send, norm_recv,
    x_send, x_recv, z_send, z_recv, f_send, f_recv,
):
    planes = groups // 2
    last = planes - 1
    feats = acts.shape[1] // groups
    width = grads.shape[1] // PIECES
    examples = acts.shape[0] // SEQ
    owned = examples // share
    me = lax.axis_index("dp")
    lane = lax.axis_index("mp")
    line, pair = me // 2, me % 2
    x_peer = {"dp": line * 2 + 1 - pair}
    above = {"dp": jnp.minimum(line + 1, last) * 2 + pair}
    below = {"dp": jnp.maximum(line - 1, 0) * 2 + pair}
    has_below = (line > 0).astype(jnp.int32)
    has_above = (line < last).astype(jnp.int32)
    part = lane % share
    first = part * owned
    away = (first + owned) % examples

    def example(i):
        return lax.rem(away + i, examples)

    def rows_of(e):
        return pl.ds(pl.multiple_of(e * SEQ, SEQ), SEQ)

    def load(e, which):
        source, target = (grads_hbm, grads) if which else (acts_hbm, acts)
        return pltpu.make_async_copy(
            source.at[rows_of(e)], target.at[rows_of(e)], load_sem.at[which, e]
        )

    for i in range(examples):
        load(example(i), 1).start()
    for i in range(examples - owned, examples):
        load(example(i), 0).start()
    for i in range(examples - owned):
        load(example(i), 0).start()

    barrier = pltpu.get_barrier_semaphore()
    pl.semaphore_signal(barrier, inc=1, device_id=x_peer, device_id_type=MESH)
    for j in range(1, lanes):
        pl.semaphore_signal(
            barrier, inc=1, device_id={"mp": lax.rem(lane + j, lanes)}, device_id_type=MESH
        )

    @pl.when(line > 0)
    def _():
        pl.semaphore_signal(barrier, inc=1, device_id=below, device_id_type=MESH)

    @pl.when(line < last)
    def _():
        pl.semaphore_signal(barrier, inc=1, device_id=above, device_id_type=MESH)

    cut = SEQ // 2

    def gram(ref, e):
        base = pl.multiple_of(e * SEQ, SEQ)
        low, high = ref[pl.ds(base, cut), :], ref[pl.ds(base + cut, cut), :]
        dot = functools.partial(
            lax.dot_general, dimension_numbers=NT, preferred_element_type=jnp.float32
        )
        return dot(low, low), dot(low, high), dot(high, high)

    def gram_copy(i):
        mate = lane - part + lax.rem(part + 1, share)
        return pltpu.make_async_remote_copy(
            src_ref=gram_mine.at[i], dst_ref=gram_peer.at[i],
            send_sem=gram_send.at[i], recv_sem=gram_recv.at[i],
            device_id={"mp": mate}, device_id_type=MESH,
        )

    if share > 1:
        def away_step(i, carry):
            e = example(i)
            load(e, 1).wait()
            for j, block in enumerate(gram(grads, e)):
                gram_mine[i, j] = block
            norm_mine[e] = jnp.zeros(norm_mine.shape[1:], jnp.float32)
            return carry

        lax.fori_loop(0, owned, away_step, 0)

    pl.semaphore_wait(barrier, lanes + has_below + has_above)
    if share > 1:
        for i in range(owned):
            gram_copy(i).start()

    def norm_step(i, carry):
        e = first + i
        load(e, 1).wait()
        gg = gram(grads, e)
        load(e, 0).wait()
        ga = gram(acts, e)
        if share > 1:
            gram_copy(i).wait_recv()
            gg = tuple(gg[j] + gram_peer[i, j] for j in range(3))
        prod = ga[0] * gg[0] + 2.0 * (ga[1] * gg[1]) + ga[2] * gg[2]
        norm_mine[e] = jnp.broadcast_to(jnp.sum(prod, keepdims=True), norm_mine.shape[1:])
        return carry

    lax.fori_loop(0, owned, norm_step, 0)

    def norm_copy(j):
        return pltpu.make_async_remote_copy(
            src_ref=norm_mine, dst_ref=norm_peer.at[j - 1],
            send_sem=norm_send.at[j - 1], recv_sem=norm_recv.at[j - 1],
            device_id={"mp": lax.rem(lane + j, lanes)}, device_id_type=MESH,
        )

    for j in range(1, lanes):
        norm_copy(j).start()

    def turn_step(e, carry):
        grads_t[:, rows_of(e)] = grads[rows_of(e), :].T
        return carry

    lax.fori_loop(0, examples, turn_step, 0)
    for i in range(examples - owned):
        load(example(i), 0).wait()
    for j in range(1, lanes):
        norm_copy(j).wait()
    if share > 1:
        for i in range(owned):
            gram_copy(i).wait_send()

    bound = bound_ref[0]
    factors = []
    for e in range(examples):
        norm_sq = norm_mine[e]
        for j in range(1, lanes):
            norm_sq = norm_sq + norm_peer[j - 1, e]
        factors.append((jnp.minimum(1.0, bound / jnp.sqrt(norm_sq + 1e-06)) / bound)[:1, :1])

    def cols_of(q):
        return pl.ds(pl.multiple_of(q * width, width), width)

    def scale(q):
        for e in range(examples):
            at = (cols_of(q), pl.ds(e * SEQ, SEQ))
            grads_t[at] = (grads_t[at].astype(jnp.float32) * factors[e]).astype(jnp.bfloat16)

    def sends_far(p):
        edge = (p == 0) | (p == last)
        up = (p < last) & ((p == 0) | (2 * p >= planes))
        down = (p > 0) & ((p == last) | (2 * p < planes))
        return up, down, jnp.where(edge, PIECES // 2, PIECES)

    far_up, far_down, far_count = sends_far(line)
    far_target = jnp.where(far_up, line + 1, line - 1)
    far_count = jnp.where(far_up | far_down, far_count, 0)

    def is_far(t, q):
        return (t == far_target) & (q < far_count)

    def arrivals_far(side, q):
        p = line - 1 if side == 0 else line + 1
        up, down, count = sends_far(p)
        exists = (line > 0) & up if side == 0 else (line < last) & down
        return exists & (q < count)

    def slot_of(t, q):
        return t * PIECES + q

    def term(block, q):
        cols = pl.ds(pl.multiple_of(block * feats, feats), feats)
        return jnp.dot(grads_t[cols_of(q), :], acts[:, cols], preferred_element_type=jnp.float32)

    def x_copy(s):
        return pltpu.make_async_remote_copy(
            src_ref=xs.at[s], dst_ref=xr.at[s], send_sem=x_send.at[s], recv_sem=x_recv.at[s],
            device_id=x_peer, device_id_type=MESH,
        )

    def z_copy(s, slot, device):
        return pltpu.make_async_remote_copy(
            src_ref=zs.at[s], dst_ref=zr.at[slot], send_sem=z_send.at[s],
            recv_sem=z_recv.at[slot], device_id=device, device_id_type=MESH,
        )

    def far_copy(q, side):
        slot = side * PIECES + q
        return pltpu.make_async_remote_copy(
            src_ref=xs.at[slot_of(far_target, q)], dst_ref=fr.at[slot], send_sem=f_send.at[q],
            recv_sem=f_recv.at[slot], device_id={"dp": far_target * 2 + pair}, device_id_type=MESH,
        )

    def target_of(k):
        ups = last - line
        up_first = jnp.where(k < ups, last - k, k - ups)
        down_first = jnp.where(k < line, k, last - (k - line))
        return jnp.where(2 * line < planes, up_first, down_first)

    def start_step(s, carry):
        @pl.when(s < PIECES)
        def _():
            scale(s)

        t, q = target_of(s // PIECES), s % PIECES

        @pl.when(jnp.logical_not(is_far(t, q)))
        def _():
            xs[slot_of(t, q)] = coded(term(t * 2 + 1 - pair, q))
            x_copy(slot_of(t, q)).start()

        @pl.when(s < far_count)
        def _():
            xs[slot_of(far_target, s)] = coded(term(far_target * 2 + 1 - pair, s))
            far_copy(s, jnp.where(far_up, 0, 1)).start()

        return carry

    lax.fori_loop(0, last * PIECES, start_step, 0)

    def pass_on(t, q, up):
        slot = slot_of(t, q)
        total[...] = term(t * 2 + pair, q)

        @pl.when(jnp.logical_not(is_far(t, q)))
        def _():
            x_copy(slot).wait_recv()
            total[...] += decoded(xr[slot])

        @pl.when(line > 0 if up else line < last)
        def _():
            z_copy(0, slot, above).wait_recv()
            total[...] += decoded(zr[slot])

        zs[slot] = coded(total[...])
        if up:
            z_copy(slot, slot, above).start()
        else:
            z_copy(slot, jnp.where(t == line - 1, planes * PIECES + q, slot), below).start()

    def pass_step(s, carry):
        i, j, k = s - line, s - (last - line), s - 2

        @pl.when((i >= 0) & (i < (last - line) * PIECES))
        def _():
            pass_on(last - i // PIECES, i % PIECES, True)

        @pl.when((j >= 0) & (j < line * PIECES))
        def _():
            pass_on(j // PIECES, j % PIECES, False)

        @pl.when((k >= 0) & (k < PIECES))
        def _():
            total[...] = term(line * 2 + 1 - pair, k)
            for side in range(2):
                @pl.when(arrivals_far(side, k))
                def _():
                    far_copy(k, side).wait_recv()
                    total[...] += decoded(fr[side * PIECES + k])

            slot = slot_of(line, k)
            xs[slot] = coded(total[...])
            x_copy(slot).start()

        return carry

    lax.fori_loop(0, max(last * PIECES, PIECES + 2), pass_step, 0)

    def out_copy(q):
        return pltpu.make_async_copy(
            out.at[:, cols_of(q)], out_hbm.at[:, cols_of(q)], out_sem.at[q]
        )

    def final_step(q, carry):
        slot = slot_of(line, q)
        total[...] = term(line * 2 + pair, q)

        @pl.when(line > 0)
        def _():
            z_copy(0, slot, above).wait_recv()
            total[...] += decoded(zr[slot])

        @pl.when(line < last)
        def _():
            z_copy(0, planes * PIECES + q, above).wait_recv()
            total[...] += decoded(zr[planes * PIECES + q])

        x_copy(slot).wait_recv()
        out[:, cols_of(q)] = (total[...] + decoded(xr[slot])).T
        out_copy(q).start()
        return carry

    lax.fori_loop(0, PIECES, final_step, 0)

    def drain_step(s, carry):
        t, q = s // PIECES, s % PIECES
        far = is_far(t, q)

        @pl.when(far)
        def _():
            far_copy(q, 0).wait_send()

        @pl.when(jnp.logical_not(far))
        def _():
            x_copy(s).wait_send()

        @pl.when(t != line)
        def _():
            z_copy(s, 0, above).wait_send()

        return carry

    lax.fori_loop(0, planes * PIECES, drain_step, 0)
    for q in range(PIECES):
        out_copy(q).wait()


def clipped_sum(act_block, grad_block, bound):
    groups, lanes = lax.axis_size("dp"), lax.axis_size("mp")
    tokens, width = act_block.shape
    cols = grad_block.shape[1]
    feats = width // groups
    slots = groups // 2 * PIECES
    examples = tokens // SEQ
    share = 2 if lanes % 2 == 0 and examples % 2 == 0 else 1
    piece = (cols // PIECES, feats)
    grams = (examples // share if share > 1 else 1, 3, SEQ // 2, SEQ // 2)
    dma = pltpu.SemaphoreType.DMA
    any_space = pl.BlockSpec(memory_space=pl.ANY)
    return pl.pallas_call(
        functools.partial(kernel, groups, lanes, share),
        out_shape=jax.ShapeDtypeStruct((feats, cols), jnp.float32),
        in_specs=[any_space, any_space, pl.BlockSpec(memory_space=pltpu.SMEM)],
        out_specs=any_space,
        scratch_shapes=[
            pltpu.VMEM((tokens, width), jnp.bfloat16),
            pltpu.VMEM((tokens, cols), jnp.bfloat16),
            pltpu.VMEM((cols, tokens), jnp.bfloat16),
            pltpu.VMEM((slots,) + piece, jnp.bfloat16),
            pltpu.VMEM((slots,) + piece, jnp.bfloat16),
            pltpu.VMEM((slots,) + piece, jnp.bfloat16),
            pltpu.VMEM((slots + PIECES,) + piece, jnp.bfloat16),
            pltpu.VMEM((2 * PIECES,) + piece, jnp.bfloat16),
            pltpu.VMEM(grams, jnp.float32),
            pltpu.VMEM(grams, jnp.float32),
            pltpu.VMEM((examples, 8, 128), jnp.float32),
            pltpu.VMEM((max(lanes - 1, 1), examples, 8, 128), jnp.float32),
            pltpu.VMEM(piece, jnp.float32),
            pltpu.VMEM((feats, cols), jnp.float32),
            dma((2, examples)),
            dma((PIECES,)),
            dma((grams[0],)),
            dma((grams[0],)),
            dma((max(lanes - 1, 1),)),
            dma((max(lanes - 1, 1),)),
            dma((slots,)),
            dma((slots,)),
            dma((slots,)),
            dma((slots + PIECES,)),
            dma((PIECES,)),
            dma((2 * PIECES,)),
        ],
        compiler_params=pltpu.CompilerParams(
            collective_id=0, has_side_effects=True, vmem_limit_bytes=60 * 2**20
        ),
        name="clipped_sum",
    )(act_block, grad_block, bound)


def on_device(acts, out_grads, clip_bound, noise):
    model_width = acts.shape[2]
    batch_total = acts.shape[1] // SEQ * lax.axis_size("dp")
    out_factor = model_width / math.sqrt(batch_total)
    updates = [
        clipped_sum(acts[g], out_grads[g], clip_bound[g : g + 1]) * out_factor + noise[g]
        for g in range(acts.shape[0])
    ]
    return jnp.stack(updates)


def solution(mesh):
    placed = (P(None, "dp", None), P(None, "dp", "mp"), P(), P(None, "dp", "mp"))
    return jax.shard_map(
        on_device, mesh=mesh, in_specs=placed, out_specs=P(None, "dp", "mp"), check_vma=False
    )
```

```python
import functools
import math

import jax
import jax.numpy as jnp
from jax import lax
from jax.experimental import pallas as pl
from jax.experimental.pallas import tpu as pltpu
from jax.sharding import PartitionSpec as P

SEQ = 512
PIECES = 4
AHEAD = PIECES
NT = (((1,), (1,)), ((), ()))
MESH = pl.DeviceIdType.MESH
LIFT = 2.0**50


def coded(value):
    lifted = value * LIFT
    return (lifted * jnp.abs(lifted)).astype(jnp.bfloat16)


def decoded(code):
    code = code.astype(jnp.float32)
    return code * lax.rsqrt(jnp.maximum(jnp.abs(code), 1e-37)) * (1.0 / LIFT)


def kernel(
    groups, lanes, share, out_factor, acts_hbm, grads_hbm, bound_ref, noise_hbm, out,
    acts, grads, grads_t, xs, xr, zs, zr, fr, gram_mine, gram_peer, gram_kept, gram_own, parts, norm_mine, norm_peer, total, noise,
    load_sem, noise_sem, gram_send, gram_recv, norm_send, norm_recv,
    x_send, x_recv, z_send, z_recv, f_send, f_recv,
):
    planes = groups // 2
    last = planes - 1
    feats = acts.shape[1] // groups
    width = grads.shape[1] // PIECES
    examples = acts.shape[0] // SEQ
    owned = examples // share
    me = lax.axis_index("dp")
    lane = lax.axis_index("mp")
    line, pair = me // 2, me % 2
    x_peer = {"dp": line * 2 + 1 - pair}
    above = {"dp": jnp.minimum(line + 1, last) * 2 + pair}
    below = {"dp": jnp.maximum(line - 1, 0) * 2 + pair}
    has_below = (line > 0).astype(jnp.int32)
    has_above = (line < last).astype(jnp.int32)
    part = lane % share
    first = part * owned
    away = (first + owned) % examples

    def example(i):
        return lax.rem(away + i, examples)

    def rows_of(e):
        return pl.ds(pl.multiple_of(e * SEQ, SEQ), SEQ)

    def load(e, which):
        source, target = (grads_hbm, grads) if which else (acts_hbm, acts)
        return pltpu.make_async_copy(
            source.at[rows_of(e)], target.at[rows_of(e)], load_sem.at[which, e]
        )

    for i in range(examples):
        load(example(i), 1).start()
    load(first, 0).start()

    barrier = pltpu.get_barrier_semaphore()
    pl.semaphore_signal(barrier, inc=1, device_id=x_peer, device_id_type=MESH)
    for j in range(1, lanes):
        pl.semaphore_signal(
            barrier, inc=1, device_id={"mp": lax.rem(lane + j, lanes)}, device_id_type=MESH
        )

    @pl.when(line > 0)
    def _():
        pl.semaphore_signal(barrier, inc=1, device_id=below, device_id_type=MESH)

    @pl.when(line < last)
    def _():
        pl.semaphore_signal(barrier, inc=1, device_id=above, device_id_type=MESH)

    def turn(e):
        grads_t[:, rows_of(e)] = grads[rows_of(e), :].T

    cut = SEQ // 2

    def gram(ref, e):
        base = pl.multiple_of(e * SEQ, SEQ)
        low, high = ref[pl.ds(base, cut), :], ref[pl.ds(base + cut, cut), :]
        dot = functools.partial(
            lax.dot_general, dimension_numbers=NT, preferred_element_type=jnp.float32
        )
        return dot(low, low), dot(low, high), dot(high, high)

    def gram_copy(i):
        mate = lane - part + lax.rem(part + 1, share)
        return pltpu.make_async_remote_copy(
            src_ref=gram_mine.at[i], dst_ref=gram_peer.at[i],
            send_sem=gram_send.at[i], recv_sem=gram_recv.at[i],
            device_id={"mp": mate}, device_id_type=MESH,
        )

    if share > 1:
        def away_step(i, carry):
            e = example(i)
            load(e, 1).wait()
            for j, block in enumerate(gram(grads, e)):
                gram_mine[i, j] = block
            return carry

        lax.fori_loop(0, owned, away_step, 0)

    def own_step(i, carry):
        load(first + i, 1).wait()
        for j, block in enumerate(gram(grads, first + i)):
            gram_own[i, j] = block
        return carry

    for i in range(1, owned):
        load(first + i, 0).start()
    lax.fori_loop(0, owned, own_step, 0)
    pl.semaphore_wait(barrier, lanes + has_below + has_above)
    if share > 1:
        for i in range(owned):
            gram_copy(i).start()

    def inner(a, b):
        prod = a[0] * b[0] + 2.0 * (a[1] * b[1]) + a[2] * b[2]
        rows = jnp.sum(prod.reshape(cut // 8, 8, cut), axis=0)
        return sum(rows[:, c : c + 128] for c in range(0, cut, 128))

    late = examples - owned
    for i in range(owned):
        e = first + i
        load(e, 0).wait()
        for j in range(i * late // owned, (i + 1) * late // owned):
            load(example(j), 0).start()
        ga = gram(acts, e)
        gg = [gram_own[i, j] for j in range(3)]
        if share > 1 and i == owned - 1:
            for k in range(owned):
                gram_copy(k).wait_recv()
            gg = [gg[j] + gram_peer[i, j] for j in range(3)]
        elif share > 1:
            for j in range(3):
                gram_kept[i, j] = ga[j]
        norm_mine[i] = inner(ga, gg)
    if share > 1:
        for i in range(owned - 1):
            norm_mine[i] += inner(gram_kept[i], gram_peer[i])

    def norm_copy(j):
        return pltpu.make_async_remote_copy(
            src_ref=norm_mine, dst_ref=norm_peer.at[j - 1],
            send_sem=norm_send.at[j - 1], recv_sem=norm_recv.at[j - 1],
            device_id={"mp": lax.rem(lane + j, lanes)}, device_id_type=MESH,
        )

    for j in range(1, lanes):
        norm_copy(j).start()

    def turn_step(e, carry):
        grads_t[:, rows_of(e)] = grads[rows_of(e), :].T
        return carry

    lax.fori_loop(0, examples, turn_step, 0)
    for i in range(late):
        load(example(i), 0).wait()

    def cols_of(q):
        return pl.ds(pl.multiple_of(q * width, width), width)

    def sends_far(p):
        edge = (p == 0) | (p == last)
        up = (p < last) & ((p == 0) | (2 * p >= planes))
        down = (p > 0) & ((p == last) | (2 * p < planes))
        return up, down, jnp.where(edge, PIECES // 2, PIECES)

    far_up, far_down, far_count = sends_far(line)
    far_target = jnp.where(far_up, line + 1, line - 1)
    far_count = jnp.where(far_up | far_down, far_count, 0)

    def is_far(t, q):
        return (t == far_target) & (q < far_count)

    def arrivals_far(side, q):
        p = line - 1 if side == 0 else line + 1
        up, down, count = sends_far(p)
        exists = (line > 0) & up if side == 0 else (line < last) & down
        return exists & (q < count)

    def slot_of(t, q):
        return t * PIECES + q

    def term(block, q):
        cols = pl.ds(pl.multiple_of(block * feats, feats), feats)
        return jnp.dot(grads_t[cols_of(q), :], acts[:, cols], preferred_element_type=jnp.float32)

    lead = jnp.where(2 * line < planes, last, 0)
    lead_q = jnp.where(is_far(lead, 0), far_count, 0)
    openers = ((lead, lead_q), (far_target, 0)) if last > 0 else ()
    for k, (t, q) in enumerate(openers):
        for e in range(examples):
            tokens = pl.ds(e * SEQ, SEQ)
            cols = pl.ds(pl.multiple_of((t * 2 + 1 - pair) * feats, feats), feats)
            parts[k, e] = jnp.dot(
                grads_t[cols_of(q), tokens], acts[tokens, cols], preferred_element_type=jnp.float32
            )

    noise_copy = pltpu.make_async_copy(noise_hbm, noise, noise_sem)
    noise_copy.start()
    for j in range(1, lanes):
        norm_copy(j).wait()

    bound = bound_ref[0]

    def factor_of(terms):
        norm_sq = jnp.sum(functools.reduce(jnp.add, terms), keepdims=True)
        return jnp.minimum(1.0, bound / jnp.sqrt(norm_sq + 1e-06)) / bound

    factors = []
    for g in range(share):
        for i in range(owned):
            same = [norm_mine[i]] + [norm_peer[j - 1, i] for j in range(share, lanes, share)]
            other = [norm_peer[j - 1, i] for j in range(1, lanes, share)]
            if share == 1:
                factors.append(factor_of(same))
            else:
                factors.append(factor_of([
                    jnp.where(part == g, a, b) for a, b in zip(same, other)
                ]))

    def scale(q):
        for e in range(examples):
            at = (cols_of(q), pl.ds(e * SEQ, SEQ))
            grads_t[at] = (grads_t[at].astype(jnp.float32) * factors[e]).astype(jnp.bfloat16)

    def x_copy(s):
        return pltpu.make_async_remote_copy(
            src_ref=xs.at[s], dst_ref=xr.at[s], send_sem=x_send.at[s], recv_sem=x_recv.at[s],
            device_id=x_peer, device_id_type=MESH,
        )

    def z_copy(s, slot, device):
        return pltpu.make_async_remote_copy(
            src_ref=zs.at[s], dst_ref=zr.at[slot], send_sem=z_send.at[s],
            recv_sem=z_recv.at[slot], device_id=device, device_id_type=MESH,
        )

    def far_copy(q, side):
        slot = side * PIECES + q
        return pltpu.make_async_remote_copy(
            src_ref=xs.at[slot_of(far_target, q)], dst_ref=fr.at[slot], send_sem=f_send.at[q],
            recv_sem=f_recv.at[slot], device_id={"dp": far_target * 2 + pair}, device_id_type=MESH,
        )

    for k, (t, q) in enumerate(openers):
        slot = slot_of(t, q)
        xs[slot] = coded(sum(parts[k, e] * factors[e] for e in range(examples)))
        if k == 0:
            x_copy(slot).start()
        else:
            far_copy(q, jnp.where(far_up, 0, 1)).start()

    def send_far(t, q):
        @pl.when(jnp.logical_not(is_far(t, q) | ((t == lead) & (q == lead_q))))
        def _():
            xs[slot_of(t, q)] = coded(term(t * 2 + 1 - pair, q))
            x_copy(slot_of(t, q)).start()

    def each(s, step):
        i, j = s - line, s - (last - line)

        @pl.when((i >= 0) & (i < (last - line) * PIECES))
        def _():
            step(last - i // PIECES, i % PIECES, True)

        @pl.when((j >= 0) & (j < line * PIECES))
        def _():
            step(j // PIECES, j % PIECES, False)

    def start_step(s, carry):
        @pl.when(s < PIECES)
        def _():
            scale(s)

        each(s, lambda t, q, up: send_far(t, q))

        @pl.when((s > 0) & (s < far_count))
        def _():
            xs[slot_of(far_target, s)] = coded(term(far_target * 2 + 1 - pair, s))
            far_copy(s, jnp.where(far_up, 0, 1)).start()

        return carry

    lax.fori_loop(0, AHEAD, start_step, 0)

    def pass_on(t, q, up):
        slot = slot_of(t, q)
        total[...] = term(t * 2 + pair, q)

        @pl.when(jnp.logical_not(is_far(t, q)))
        def _():
            x_copy(slot).wait_recv()
            total[...] += decoded(xr[slot])

        @pl.when(line > 0 if up else line < last)
        def _():
            z_copy(0, slot, above).wait_recv()
            total[...] += decoded(zr[slot])

        zs[slot] = coded(total[...])
        if up:
            z_copy(slot, slot, above).start()
        else:
            z_copy(slot, jnp.where(t == line - 1, planes * PIECES + q, slot), below).start()

    edge = (line == 0) | (line == last)
    opens = jnp.maximum(last * PIECES - AHEAD - jnp.where(edge, 0, PIECES), 0)

    def pass_step(s, carry):
        k = s - opens
        each(s + AHEAD, lambda t, q, up: send_far(t, q))
        each(s, pass_on)

        @pl.when((k >= 0) & (k < PIECES))
        def _():
            total[...] = term(line * 2 + 1 - pair, k)
            for side in range(2):
                @pl.when(arrivals_far(side, k))
                def _():
                    far_copy(k, side).wait_recv()
                    total[...] += decoded(fr[side * PIECES + k])

            slot = slot_of(line, k)
            xs[slot] = coded(total[...])
            x_copy(slot).start()

        return carry

    lax.fori_loop(0, max(last, 1) * PIECES, pass_step, 0)

    noise_copy.wait()

    def final_step(q, carry):
        slot = slot_of(line, q)
        total[...] = term(line * 2 + pair, q)

        @pl.when(line > 0)
        def _():
            z_copy(0, slot, above).wait_recv()
            total[...] += decoded(zr[slot])

        @pl.when(line < last)
        def _():
            z_copy(0, planes * PIECES + q, above).wait_recv()
            total[...] += decoded(zr[planes * PIECES + q])

        x_copy(slot).wait_recv()
        summed = (total[...] + decoded(xr[slot])).T
        out[:, cols_of(q)] = summed * out_factor + noise[:, cols_of(q)]
        return carry

    lax.fori_loop(0, PIECES, final_step, 0)

    def drain_step(s, carry):
        t, q = s // PIECES, s % PIECES
        far = is_far(t, q)

        @pl.when(far)
        def _():
            far_copy(q, 0).wait_send()

        @pl.when(jnp.logical_not(far))
        def _():
            x_copy(s).wait_send()

        @pl.when(t != line)
        def _():
            z_copy(s, 0, above).wait_send()

        return carry

    lax.fori_loop(0, planes * PIECES, drain_step, 0)
    if share > 1:
        for i in range(owned):
            gram_copy(i).wait_send()


def clipped_sum(act_block, grad_block, bound, noise, out_factor):
    groups, lanes = lax.axis_size("dp"), lax.axis_size("mp")
    tokens, width = act_block.shape
    cols = grad_block.shape[1]
    feats = width // groups
    slots = groups // 2 * PIECES
    examples = tokens // SEQ
    share = 2 if lanes % 2 == 0 and examples % 2 == 0 else 1
    piece = (cols // PIECES, feats)
    grams = (examples // share if share > 1 else 1, 3, SEQ // 2, SEQ // 2)
    dma = pltpu.SemaphoreType.DMA
    any_space = pl.BlockSpec(memory_space=pl.ANY)
    return pl.pallas_call(
        functools.partial(kernel, groups, lanes, share, out_factor),
        out_shape=pltpu.VMEM((feats, cols), jnp.float32),
        in_specs=[any_space, any_space, pl.BlockSpec(memory_space=pltpu.SMEM), any_space],
        out_specs=pl.BlockSpec(memory_space=pltpu.VMEM),
        scratch_shapes=[
            pltpu.VMEM((tokens, width), jnp.bfloat16),
            pltpu.VMEM((tokens, cols), jnp.bfloat16),
            pltpu.VMEM((cols, tokens), jnp.bfloat16),
            pltpu.VMEM((slots,) + piece, jnp.bfloat16),
            pltpu.VMEM((slots,) + piece, jnp.bfloat16),
            pltpu.VMEM((slots,) + piece, jnp.bfloat16),
            pltpu.VMEM((slots + PIECES,) + piece, jnp.bfloat16),
            pltpu.VMEM((2 * PIECES,) + piece, jnp.bfloat16),
            pltpu.VMEM(grams, jnp.float32),
            pltpu.VMEM(grams, jnp.float32),
            pltpu.VMEM(grams, jnp.float32),
            pltpu.VMEM((examples // share,) + grams[1:], jnp.float32),
            pltpu.VMEM((2, examples) + piece, jnp.float32),
            pltpu.VMEM((examples // share, 8, 128), jnp.float32),
            pltpu.VMEM((max(lanes - 1, 1), examples // share, 8, 128), jnp.float32),
            pltpu.VMEM(piece, jnp.float32),
            pltpu.VMEM((feats, cols), jnp.float32),
            dma((2, examples)),
            dma(()),
            dma((grams[0],)),
            dma((grams[0],)),
            dma((max(lanes - 1, 1),)),
            dma((max(lanes - 1, 1),)),
            dma((slots,)),
            dma((slots,)),
            dma((slots,)),
            dma((slots + PIECES,)),
            dma((PIECES,)),
            dma((2 * PIECES,)),
        ],
        compiler_params=pltpu.CompilerParams(
            collective_id=0, has_side_effects=True, vmem_limit_bytes=61 * 2**20
        ),
        name="clipped_sum",
    )(act_block, grad_block, bound, noise)


def on_device(acts, out_grads, clip_bound, noise):
    model_width = acts.shape[2]
    batch_total = acts.shape[1] // SEQ * lax.axis_size("dp")
    out_factor = model_width / math.sqrt(batch_total)
    updates = [
        clipped_sum(acts[g], out_grads[g], clip_bound[g : g + 1], noise[g], out_factor)
        for g in range(acts.shape[0])
    ]
    return jnp.stack(updates)


def solution(mesh):
    placed = (P(None, "dp", None), P(None, "dp", "mp"), P(), P(None, "dp", "mp"))
    return jax.shard_map(
        on_device, mesh=mesh, in_specs=placed, out_specs=P(None, "dp", "mp"), check_vma=False
    )
```

```python
import functools
import math

import jax
import jax.numpy as jnp
from jax import lax
from jax.experimental import pallas as pl
from jax.experimental.pallas import tpu as pltpu
from jax.sharding import PartitionSpec as P

SEQ = 512
PIECES = 4
AHEAD = PIECES
NT = (((1,), (1,)), ((), ()))
MESH = pl.DeviceIdType.MESH
LIFT = 2.0**50


def coded(value):
    lifted = value * LIFT
    return (lifted * jnp.abs(lifted)).astype(jnp.bfloat16)


def decoded(code):
    code = code.astype(jnp.float32)
    return code * lax.rsqrt(jnp.maximum(jnp.abs(code), 1e-37)) * (1.0 / LIFT)


def kernel(
    groups, lanes, share, out_factor, acts_hbm, grads_hbm, bound_ref, noise_hbm, out,
    acts, grads, grads_t, xs, xr, zs, zr, fr, gram_mine, gram_peer, gram_kept, gram_own, parts, norm_mine, norm_peer, total, noise,
    load_sem, noise_sem, gram_send, gram_recv, norm_send, norm_recv,
    x_send, x_recv, z_send, z_recv, f_send, f_recv,
):
    planes = groups // 2
    last = planes - 1
    feats = acts.shape[1] // groups
    width = grads.shape[1] // PIECES
    examples = acts.shape[0] // SEQ
    owned = examples // share
    me = lax.axis_index("dp")
    lane = lax.axis_index("mp")
    line, pair = me // 2, me % 2
    x_peer = {"dp": line * 2 + 1 - pair}
    above = {"dp": jnp.minimum(line + 1, last) * 2 + pair}
    below = {"dp": jnp.maximum(line - 1, 0) * 2 + pair}
    has_below = (line > 0).astype(jnp.int32)
    has_above = (line < last).astype(jnp.int32)
    part = lane % share
    first = part * owned
    away = (first + owned) % examples

    def example(i):
        return lax.rem(away + i, examples)

    def rows_of(e):
        return pl.ds(pl.multiple_of(e * SEQ, SEQ), SEQ)

    def load(e, which):
        source, target = (grads_hbm, grads) if which else (acts_hbm, acts)
        return pltpu.make_async_copy(
            source.at[rows_of(e)], target.at[rows_of(e)], load_sem.at[which, e]
        )

    for i in range(examples):
        load(example(i), 1).start()
    load(first, 0).start()

    barrier = pltpu.get_barrier_semaphore()
    pl.semaphore_signal(barrier, inc=1, device_id=x_peer, device_id_type=MESH)
    for j in range(1, lanes):
        pl.semaphore_signal(
            barrier, inc=1, device_id={"mp": lax.rem(lane + j, lanes)}, device_id_type=MESH
        )

    @pl.when(line > 0)
    def _():
        pl.semaphore_signal(barrier, inc=1, device_id=below, device_id_type=MESH)

    @pl.when(line < last)
    def _():
        pl.semaphore_signal(barrier, inc=1, device_id=above, device_id_type=MESH)

    def turn(e):
        grads_t[:, rows_of(e)] = grads[rows_of(e), :].T

    cut = SEQ // 2

    def gram(ref, e):
        base = pl.multiple_of(e * SEQ, SEQ)
        low, high = ref[pl.ds(base, cut), :], ref[pl.ds(base + cut, cut), :]
        dot = functools.partial(
            lax.dot_general, dimension_numbers=NT, preferred_element_type=jnp.float32
        )
        return dot(low, low), dot(low, high), dot(high, high)

    def gram_copy(i):
        mate = lane - part + lax.rem(part + 1, share)
        return pltpu.make_async_remote_copy(
            src_ref=gram_mine.at[i], dst_ref=gram_peer.at[i],
            send_sem=gram_send.at[i], recv_sem=gram_recv.at[i],
            device_id={"mp": mate}, device_id_type=MESH,
        )

    if share > 1:
        def away_step(i, carry):
            e = example(i)
            load(e, 1).wait()
            for j, block in enumerate(gram(grads, e)):
                gram_mine[i, j] = block
            return carry

        lax.fori_loop(0, owned, away_step, 0)

    def own_step(i, carry):
        load(first + i, 1).wait()
        for j, block in enumerate(gram(grads, first + i)):
            gram_own[i, j] = block
        return carry

    for i in range(1, owned):
        load(first + i, 0).start()
    lax.fori_loop(0, owned, own_step, 0)
    pl.semaphore_wait(barrier, lanes + has_below + has_above)
    if share > 1:
        for i in range(owned):
            gram_copy(i).start()

    def inner(a, b):
        prod = a[0] * b[0] + 2.0 * (a[1] * b[1]) + a[2] * b[2]
        rows = jnp.sum(prod.reshape(cut // 8, 8, cut), axis=0)
        return sum(rows[:, c : c + 128] for c in range(0, cut, 128))

    late = examples - owned
    for i in range(owned):
        e = first + i
        load(e, 0).wait()
        for j in range(i * late // owned, (i + 1) * late // owned):
            load(example(j), 0).start()
        ga = gram(acts, e)
        gg = [gram_own[i, j] for j in range(3)]
        if share > 1 and i == owned - 1:
            for k in range(owned):
                gram_copy(k).wait_recv()
            gg = [gg[j] + gram_peer[i, j] for j in range(3)]
        elif share > 1:
            for j in range(3):
                gram_kept[i, j] = ga[j]
        norm_mine[i] = inner(ga, gg)
    if share > 1:
        for i in range(owned - 1):
            norm_mine[i] += inner(gram_kept[i], gram_peer[i])

    def norm_copy(j):
        return pltpu.make_async_remote_copy(
            src_ref=norm_mine, dst_ref=norm_peer.at[j - 1],
            send_sem=norm_send.at[j - 1], recv_sem=norm_recv.at[j - 1],
            device_id={"mp": lax.rem(lane + j, lanes)}, device_id_type=MESH,
        )

    for j in sorted(range(1, lanes), key=lambda j: -(j % 2 == 0)):
        norm_copy(j).start()

    def turn_step(e, carry):
        grads_t[:, rows_of(e)] = grads[rows_of(e), :].T
        return carry

    lax.fori_loop(0, examples, turn_step, 0)
    for i in range(late):
        load(example(i), 0).wait()

    def cols_of(q):
        return pl.ds(pl.multiple_of(q * width, width), width)

    def sends_far(p):
        edge = (p == 0) | (p == last)
        up = (p < last) & ((p == 0) | (2 * p >= planes))
        down = (p > 0) & ((p == last) | (2 * p < planes))
        return up, down, jnp.where(edge, PIECES // 2, PIECES)

    far_up, far_down, far_count = sends_far(line)
    far_target = jnp.where(far_up, line + 1, line - 1)
    far_count = jnp.where(far_up | far_down, far_count, 0)

    def is_far(t, q):
        return (t == far_target) & (q < far_count)

    def arrivals_far(side, q):
        p = line - 1 if side == 0 else line + 1
        up, down, count = sends_far(p)
        exists = (line > 0) & up if side == 0 else (line < last) & down
        return exists & (q < count)

    def slot_of(t, q):
        return t * PIECES + q

    def term(block, q):
        cols = pl.ds(pl.multiple_of(block * feats, feats), feats)
        return jnp.dot(grads_t[cols_of(q), :], acts[:, cols], preferred_element_type=jnp.float32)

    lead = jnp.where(2 * line < planes, last, 0)
    lead_q = jnp.where(is_far(lead, 0), far_count, 0)
    openers = ((lead, lead_q), (far_target, 0)) if last > 0 else ()
    for k, (t, q) in enumerate(openers):
        for e in range(examples):
            tokens = pl.ds(e * SEQ, SEQ)
            cols = pl.ds(pl.multiple_of((t * 2 + 1 - pair) * feats, feats), feats)
            parts[k, e] = jnp.dot(
                grads_t[cols_of(q), tokens], acts[tokens, cols], preferred_element_type=jnp.float32
            )

    noise_copy = pltpu.make_async_copy(noise_hbm, noise, noise_sem)
    noise_copy.start()
    for j in range(1, lanes):
        norm_copy(j).wait_recv()

    bound = bound_ref[0]

    def factor_of(terms):
        norm_sq = jnp.sum(functools.reduce(jnp.add, terms), keepdims=True)
        return jnp.minimum(1.0, bound / jnp.sqrt(norm_sq + 1e-06)) / bound

    factors = []
    for g in range(share):
        for i in range(owned):
            same = [norm_mine[i]] + [norm_peer[j - 1, i] for j in range(share, lanes, share)]
            other = [norm_peer[j - 1, i] for j in range(1, lanes, share)]
            if share == 1:
                factors.append(factor_of(same))
            else:
                factors.append(factor_of([
                    jnp.where(part == g, a, b) for a, b in zip(same, other)
                ]))

    def scale(q):
        for e in range(examples):
            at = (cols_of(q), pl.ds(e * SEQ, SEQ))
            grads_t[at] = (grads_t[at].astype(jnp.float32) * factors[e]).astype(jnp.bfloat16)

    def x_copy(s):
        return pltpu.make_async_remote_copy(
            src_ref=xs.at[s], dst_ref=xr.at[s], send_sem=x_send.at[s], recv_sem=x_recv.at[s],
            device_id=x_peer, device_id_type=MESH,
        )

    def z_copy(s, slot, device):
        return pltpu.make_async_remote_copy(
            src_ref=zs.at[s], dst_ref=zr.at[slot], send_sem=z_send.at[s],
            recv_sem=z_recv.at[slot], device_id=device, device_id_type=MESH,
        )

    def far_copy(q, side):
        slot = side * PIECES + q
        return pltpu.make_async_remote_copy(
            src_ref=xs.at[slot_of(far_target, q)], dst_ref=fr.at[slot], send_sem=f_send.at[q],
            recv_sem=f_recv.at[slot], device_id={"dp": far_target * 2 + pair}, device_id_type=MESH,
        )

    for k, (t, q) in enumerate(openers):
        slot = slot_of(t, q)
        xs[slot] = coded(sum(parts[k, e] * factors[e] for e in range(examples)))
        if k == 0:
            x_copy(slot).start()
        else:
            far_copy(q, jnp.where(far_up, 0, 1)).start()

    def send_far(t, q):
        @pl.when(jnp.logical_not(is_far(t, q) | ((t == lead) & (q == lead_q))))
        def _():
            xs[slot_of(t, q)] = coded(term(t * 2 + 1 - pair, q))
            x_copy(slot_of(t, q)).start()

    def each(s, step):
        i, j = s - line, s - (last - line)

        @pl.when((i >= 0) & (i < (last - line) * PIECES))
        def _():
            step(last - i // PIECES, i % PIECES, True)

        @pl.when((j >= 0) & (j < line * PIECES))
        def _():
            step(j // PIECES, j % PIECES, False)

    def start_step(s, carry):
        @pl.when(s < PIECES)
        def _():
            scale(s)

        each(s, lambda t, q, up: send_far(t, q))

        @pl.when((s > 0) & (s < far_count))
        def _():
            xs[slot_of(far_target, s)] = coded(term(far_target * 2 + 1 - pair, s))
            far_copy(s, jnp.where(far_up, 0, 1)).start()

        return carry

    lax.fori_loop(0, AHEAD, start_step, 0)

    def pass_on(t, q, up):
        slot = slot_of(t, q)
        total[...] = term(t * 2 + pair, q)

        @pl.when(jnp.logical_not(is_far(t, q)))
        def _():
            x_copy(slot).wait_recv()
            total[...] += decoded(xr[slot])

        @pl.when(line > 0 if up else line < last)
        def _():
            z_copy(0, slot, above).wait_recv()
            total[...] += decoded(zr[slot])

        zs[slot] = coded(total[...])
        if up:
            z_copy(slot, slot, above).start()
        else:
            z_copy(slot, jnp.where(t == line - 1, planes * PIECES + q, slot), below).start()

    edge = (line == 0) | (line == last)
    opens = jnp.maximum(last * PIECES - AHEAD - jnp.where(edge, 0, PIECES), 0)

    def pass_step(s, carry):
        k = s - opens
        each(s + AHEAD, lambda t, q, up: send_far(t, q))
        each(s, pass_on)

        @pl.when((k >= 0) & (k < PIECES))
        def _():
            total[...] = term(line * 2 + 1 - pair, k)
            for side in range(2):
                @pl.when(arrivals_far(side, k))
                def _():
                    far_copy(k, side).wait_recv()
                    total[...] += decoded(fr[side * PIECES + k])

            slot = slot_of(line, k)
            xs[slot] = coded(total[...])
            x_copy(slot).start()

        return carry

    lax.fori_loop(0, max(last, 1) * PIECES, pass_step, 0)

    noise_copy.wait()

    def final_step(q, carry):
        slot = slot_of(line, q)
        total[...] = term(line * 2 + pair, q)

        @pl.when(line > 0)
        def _():
            z_copy(0, slot, above).wait_recv()
            total[...] += decoded(zr[slot])

        @pl.when(line < last)
        def _():
            z_copy(0, planes * PIECES + q, above).wait_recv()
            total[...] += decoded(zr[planes * PIECES + q])

        x_copy(slot).wait_recv()
        summed = (total[...] + decoded(xr[slot])).T
        out[:, cols_of(q)] = summed * out_factor + noise[:, cols_of(q)]
        return carry

    def drain_step(s, carry):
        t, q = s // PIECES, s % PIECES
        far = is_far(t, q)

        @pl.when(far)
        def _():
            far_copy(q, 0).wait_send()

        @pl.when(jnp.logical_not(far))
        def _():
            x_copy(s).wait_send()

        @pl.when(t != line)
        def _():
            z_copy(s, 0, above).wait_send()

        return carry

    def drain():
        lax.fori_loop(0, planes * PIECES, drain_step, 0)
        for j in range(1, lanes):
            norm_copy(j).wait_send()
        if share > 1:
            for i in range(owned):
                gram_copy(i).wait_send()

    lax.fori_loop(0, PIECES - 1, final_step, 0)
    drain()
    final_step(PIECES - 1, 0)


def clipped_sum(act_block, grad_block, bound, noise, out_factor):
    groups, lanes = lax.axis_size("dp"), lax.axis_size("mp")
    tokens, width = act_block.shape
    cols = grad_block.shape[1]
    feats = width // groups
    slots = groups // 2 * PIECES
    examples = tokens // SEQ
    share = 2 if lanes % 2 == 0 and examples % 2 == 0 else 1
    piece = (cols // PIECES, feats)
    grams = (examples // share if share > 1 else 1, 3, SEQ // 2, SEQ // 2)
    dma = pltpu.SemaphoreType.DMA
    any_space = pl.BlockSpec(memory_space=pl.ANY)
    return pl.pallas_call(
        functools.partial(kernel, groups, lanes, share, out_factor),
        out_shape=pltpu.VMEM((feats, cols), jnp.float32),
        in_specs=[any_space, any_space, pl.BlockSpec(memory_space=pltpu.SMEM), any_space],
        out_specs=pl.BlockSpec(memory_space=pltpu.VMEM),
        scratch_shapes=[
            pltpu.VMEM((tokens, width), jnp.bfloat16),
            pltpu.VMEM((tokens, cols), jnp.bfloat16),
            pltpu.VMEM((cols, tokens), jnp.bfloat16),
            pltpu.VMEM((slots,) + piece, jnp.bfloat16),
            pltpu.VMEM((slots,) + piece, jnp.bfloat16),
            pltpu.VMEM((slots,) + piece, jnp.bfloat16),
            pltpu.VMEM((slots + PIECES,) + piece, jnp.bfloat16),
            pltpu.VMEM((2 * PIECES,) + piece, jnp.bfloat16),
            pltpu.VMEM(grams, jnp.float32),
            pltpu.VMEM(grams, jnp.float32),
            pltpu.VMEM(grams, jnp.float32),
            pltpu.VMEM((examples // share,) + grams[1:], jnp.float32),
            pltpu.VMEM((2, examples) + piece, jnp.float32),
            pltpu.VMEM((examples // share, 8, 128), jnp.float32),
            pltpu.VMEM((max(lanes - 1, 1), examples // share, 8, 128), jnp.float32),
            pltpu.VMEM(piece, jnp.float32),
            pltpu.VMEM((feats, cols), jnp.float32),
            dma((2, examples)),
            dma(()),
            dma((grams[0],)),
            dma((grams[0],)),
            dma((max(lanes - 1, 1),)),
            dma((max(lanes - 1, 1),)),
            dma((slots,)),
            dma((slots,)),
            dma((slots,)),
            dma((slots + PIECES,)),
            dma((PIECES,)),
            dma((2 * PIECES,)),
        ],
        compiler_params=pltpu.CompilerParams(
            collective_id=0, has_side_effects=True, vmem_limit_bytes=61 * 2**20
        ),
        name="clipped_sum",
    )(act_block, grad_block, bound, noise)


def on_device(acts, out_grads, clip_bound, noise):
    model_width = acts.shape[2]
    batch_total = acts.shape[1] // SEQ * lax.axis_size("dp")
    out_factor = model_width / math.sqrt(batch_total)
    updates = [
        clipped_sum(acts[g], out_grads[g], clip_bound[g : g + 1], noise[g], out_factor)
        for g in range(acts.shape[0])
    ]
    return jnp.stack(updates)


def solution(mesh):
    placed = (P(None, "dp", None), P(None, "dp", "mp"), P(), P(None, "dp", "mp"))
    return jax.shard_map(
        on_device, mesh=mesh, in_specs=placed, out_specs=P(None, "dp", "mp"), check_vma=False
    )
```
